32 devices in a mesh: vblk: 4 (over y, x), samp: 8 (over z, core).
Axes of the slice: x: 2, y: 2, z: 4, core: 2. Of those that a mesh axis runs over, the one named last changes fastest.
Arguments:
- vectors: bfloat16 [1024, 32768], P('vblk', 'samp'), may hold values from 0 to 2, as said below
- partner: bfloat16 [1024, 32768], P('vblk', 'samp'), may hold values from 0 to 2, as said below
- next_rows: bfloat16 [1024, 32768], P(('vblk', 'samp')), may hold values from 0 to 2, as said below
Outputs:
- metric: float32 [1024, 256], P('vblk', 'samp')
- next_block: bfloat16 [1024, 32768], P('vblk', 'samp')
The draws below stay inside these ranges and needn't reach their ends.
Inputs may be any that keep to these rules, and one draw needn't show every extreme that they name: vectors: real expected allele dosages, every entry positive. partner: real expected allele dosages, every entry positive. next_rows: real expected allele dosages, every entry positive.
All inputs are finite; a program needn't handle non-finite values.
Results may differ from the reference program's by a relative error of at most 0.0004.
Values may be sent and summed in bfloat16 or wider, within the bound.
No kernel may reach another device: no remote copies, remote signals or barrier semaphores. Data moves between devices by JAX's collectives and lax.ppermute only.
A program may use at most 64 MiB of HBM per device.

```python
import math
import jax
import jax.numpy as jnp
from jax import lax

NSAMP = 32768
NVD = 256
NVEC = 1024
NXVEC = 1024
N_VBLK = 4
N_SAMP = 8


def shard_factor(key, salt_value, low_value):
    key = jax.random.fold_in(key, salt_value)
    factors = jnp.exp(jax.random.uniform(key, (N_SAMP,), jnp.float32, math.log(low_value), 0.0))
    return jnp.repeat(factors, NSAMP // N_SAMP)[None, :]


def dosage(key, salt_value, row_count):
    common = shard_factor(key, 20, 1.0 / 30.0)
    if salt_value == 13:
        own_factor = jnp.ones((1, NSAMP), jnp.float32)
    else:
        own_factor = shard_factor(key, 20 + salt_value, 0.03)
    key = jax.random.fold_in(key, salt_value)
    subkeys = jax.random.split(key, 3)
    low = math.log(0.1)
    row_scale = jnp.exp(jax.random.uniform(subkeys[0], (row_count, 1), jnp.float32, low, 0.0))
    sample_ramp = (1.0 + 2.0 * jnp.arange(NSAMP, dtype=jnp.float32) / (NSAMP - 1)) / 3.0
    col_scale = jnp.exp(jax.random.uniform(subkeys[1], (1, NSAMP), jnp.float32, low, 0.0)) * sample_ramp[None, :]
    col_scale = col_scale * common * own_factor
    raw_values = jax.random.uniform(subkeys[2], (row_count, NSAMP), jnp.float32, 0.05, 1.0)
    return (2.0 * row_scale * col_scale * raw_values).astype(jnp.bfloat16)


def draw_vectors(key, part):
    return dosage(key, 11, NVEC)


def draw_partner(key, part):
    return dosage(key, 12, NVEC)


def draw_next_rows(key, part):
    return dosage(key, 13, NXVEC)


def setup_inputs(seed: int = 0) -> dict:
    arg_keys = jax.random.split(jax.random.key(seed), 4)
    return {
        "vectors": draw_vectors(jax.random.fold_in(arg_keys[3], 71), 0),
        "partner": draw_partner(jax.random.fold_in(arg_keys[3], 71), 0),
        "next_rows": draw_next_rows(jax.random.fold_in(arg_keys[3], 71), 0),
    }


def block_metric(own_block, pair_block):
    row_count = own_block.shape[0]
    grouped = own_block.reshape(row_count // 8, 8, own_block.shape[1])
    pair_wide = pair_block.astype(jnp.float32)

    def group_sums(row_group):
        return jnp.sum(jnp.minimum(row_group.astype(jnp.float32)[:, None, :], pair_wide[None, :, :]), axis=2)

    numerators = lax.map(group_sums, grouped).reshape(row_count, pair_block.shape[0])
    own_totals = jnp.sum(own_block.astype(jnp.float32), axis=1)
    pair_totals = jnp.sum(pair_wide, axis=1)
    return 2.0 * numerators / (own_totals[:, None] + pair_totals[None, :])


def reference(vectors, partner, next_rows):
    own_blocks = vectors.reshape(N_VBLK, NVD, NSAMP)
    pair_blocks = jnp.roll(partner.reshape(N_VBLK, NVD, NSAMP), 1, axis=0)
    metric = lax.map(lambda paired: block_metric(paired[0], paired[1]), (own_blocks, pair_blocks))
    return metric.reshape(NVEC, NVD), next_rows
```

```python
import jax
import jax.numpy as jnp
from jax import lax
from jax.experimental import pallas as pl
from jax.experimental.pallas import tpu as pltpu
from jax.sharding import PartitionSpec as P

F32 = jnp.float32
BF16 = jnp.bfloat16
CHUNKS = 8
DEPTH = 8


def from_behind(value, axis, steps):
    count = lax.axis_size(axis)
    pairs = [(source, (source + steps) % count) for source in range(count)]
    return lax.ppermute(value, axis, pairs)


def tree_sum(terms):
    while len(terms) > 1:
        paired = [terms[i] + terms[i + 1] for i in range(0, len(terms) - 1, 2)]
        terms = paired + terms[len(paired) * 2 :]
    return terms[0]


def largest_divisor(size, limit):
    return max(d for d in range(1, limit + 1) if size % d == 0)


def lane_sums(left, right):
    return lax.dot_general(left, right, (((1,), (1,)), ((), ())), preferred_element_type=F32)


def chunk_terms(cols, rows):
    col_count, samples = cols.shape
    row_count = rows.shape[0]
    halves = 2 if samples % 512 == 0 else 1
    span = samples // halves
    depth = largest_divisor(span // 128, DEPTH)
    width = span // depth
    group = 2 if col_count % 2 == 0 else 1

    def kernel(col_ref, row_ref, out_ref, total_ref, wide_ref):
        wide_ref[...] = col_ref[...].astype(F32)
        total_ref[...] = lane_sums(jnp.ones((8, samples), BF16), col_ref[...])
        ones = jnp.ones((8, width), BF16)

        def step(index, carry):
            sums = [[] for _ in range(group)]
            for half in range(halves):
                start = half * span
                spread = [
                    jnp.broadcast_to(
                        wide_ref[pl.ds(index * group + q, 1), start : start + span], (16, span)
                    ).astype(BF16)
                    for q in range(group)
                ]
                parts = [[] for _ in range(group)]
                for block in range(0, row_count, 16):
                    for q in range(group):
                        parts[q].append(
                            tree_sum(
                                [
                                    jnp.minimum(
                                        row_ref[block : block + 16, start + k : start + k + width],
                                        spread[q][:, k : k + width],
                                    )
                                    for k in range(0, span, width)
                                ]
                            )
                        )
                for q in range(group):
                    sums[q].append(lane_sums(ones, jnp.concatenate(parts[q], 0)))
            for q in range(group):
                out_ref[pl.ds(index * group + q, 1), :] = tree_sum(sums[q])[0:1]
            return carry

        lax.fori_loop(0, col_count // group, step, 0)

    vmem = pl.BlockSpec(memory_space=pltpu.VMEM)
    return pl.pallas_call(
        kernel,
        out_shape=(
            jax.ShapeDtypeStruct((col_count, row_count), F32),
            jax.ShapeDtypeStruct((8, col_count), F32),
        ),
        in_specs=[vmem, vmem],
        out_specs=(vmem, vmem),
        scratch_shapes=[pltpu.VMEM((col_count, samples), F32)],
        name="chunk_terms",
    )(cols, rows)


def body(vectors, partner, next_rows):
    shards = lax.axis_size("samp")
    row_count = vectors.shape[0]
    col_count = partner.shape[0]
    chunk = col_count // CHUNKS
    arrived = [
        from_behind(partner[i * chunk : (i + 1) * chunk], "vblk", 1) for i in range(CHUNKS)
    ]
    samples = next_rows.shape[1] // shards
    outgoing = next_rows.reshape(next_rows.shape[0], shards, samples).transpose(1, 0, 2)
    next_block = lax.all_to_all(outgoing, "samp", split_axis=0, concat_axis=0, tiled=True)
    next_block = next_block.reshape(-1, samples)

    row_totals = jnp.sum(vectors, axis=1, dtype=F32)
    arrived[-1], next_block = lax.optimization_barrier((arrived[-1], next_block))
    terms = [chunk_terms(piece, vectors) for piece in arrived]
    numerators = jnp.concatenate([t[0] for t in terms], 0)
    col_totals = jnp.concatenate([t[1][0] for t in terms], 0)
    own = col_count // shards
    payload = jnp.concatenate(
        [
            numerators.reshape(shards, own, row_count),
            jnp.broadcast_to(row_totals[None, None, :], (shards, 1, row_count)),
            jnp.pad(col_totals.reshape(shards, 1, own), ((0, 0), (0, 0), (0, row_count - own))),
        ],
        axis=1,
    )
    payload = jnp.pad(payload, ((0, 0), (0, -payload.shape[1] % 8), (0, 0)))
    summed = jnp.sum(
        lax.all_to_all(payload, "samp", split_axis=0, concat_axis=0, tiled=True), axis=0
    )
    metric = 2.0 * summed[:own] / (summed[own][None, :] + summed[own + 1, :own][:, None])
    return (metric.T, next_block)


def solution(mesh):
    in_specs = (P("vblk", "samp"), P("vblk", "samp"), P(("vblk", "samp"), None))
    out_specs = (P("vblk", "samp"), P("vblk", "samp"))
    return jax.shard_map(body, mesh=mesh, in_specs=in_specs, out_specs=out_specs, check_vma=False)
```

```python
import jax
import jax.numpy as jnp
from jax import lax
from jax.experimental import pallas as pl
from jax.experimental.pallas import tpu as pltpu
from jax.sharding import PartitionSpec as P


F32 = jnp.float32
BF16 = jnp.bfloat16
CUTS = (0, 2, 6, 11, 16)
DEPTH = 8


def from_behind(value, axis, steps):
    count = lax.axis_size(axis)
    pairs = [(source, (source + steps) % count) for source in range(count)]
    return lax.ppermute(value, axis, pairs)


def tree_sum(terms):
    while len(terms) > 1:
        paired = [terms[i] + terms[i + 1] for i in range(0, len(terms) - 1, 2)]
        terms = paired + terms[len(paired) * 2 :]
    return terms[0]


def largest_divisor(size, limit):
    return max(d for d in range(1, limit + 1) if size % d == 0)


def lane_sums(left, right):
    return lax.dot_general(left, right, (((1,), (1,)), ((), ())), preferred_element_type=F32)


def chunk_terms(cols, rows, first, payload, totals, landed):
    col_count, samples = cols.shape
    row_count = rows.shape[0]
    shards, height, _ = payload if isinstance(payload, tuple) else payload.shape
    own = totals[2]
    last = totals[0] is not None
    halves = 2 if samples % 512 == 0 else 1
    span = samples // halves
    depth = largest_divisor(span // 128, DEPTH)
    width = span // depth
    group = 2
    steps = col_count // group
    slot_width = group * halves * width
    chained = not isinstance(payload, tuple)

    def kernel(*refs):
        refs = list(refs)
        col_ref, row_ref = refs[:2]
        refs = refs[2:]
        old_ref = refs.pop(0) if chained else None
        if last:
            row_total_ref, col_total_ref, landed_ref = refs[:3]
            refs = refs[3:]
        out_ref = refs.pop(0)
        if last:
            moved_ref = refs.pop(0)
        wide_ref, part_ref = refs[:2]
        if last:
            move = pltpu.make_async_copy(landed_ref, moved_ref, refs[2])
            move.start()
        wide_ref[...] = col_ref[...].astype(F32)
        if chained:
            out_ref[...] = old_ref[...]
        else:
            out_ref[...] = jnp.zeros_like(out_ref)
        ones = jnp.ones((8, halves * width), BF16)

        def minima(step, slot):
            for half in range(halves):
                start = half * span
                spread = [
                    jnp.broadcast_to(
                        wide_ref[pl.ds(step * group + q, 1), start : start + span], (16, span)
                    ).astype(BF16)
                    for q in range(group)
                ]
                for block in range(0, row_count, 16):
                    for q in range(group):
                        at = slot * slot_width + (q * halves + half) * width
                        part_ref[block : block + 16, at : at + width] = tree_sum(
                            [
                                jnp.minimum(
                                    row_ref[block : block + 16, start + k : start + k + width],
                                    spread[q][:, k : k + width],
                                )
                                for k in range(0, span, width)
                            ]
                        )

        def finish(step, slot):
            for q in range(group):
                at = slot * slot_width + q * halves * width
                line = lane_sums(ones, part_ref[:, at : at + halves * width])
                col = first + step * group + q
                out_ref[col // own, pl.ds(col % own, 1), :] = line[0:1]

        minima(0, 0)

        def two_steps(index, carry):
            finish(2 * index, 0)
            minima(2 * index + 1, 1)
            finish(2 * index + 1, 1)
            minima(jnp.minimum(2 * index + 2, steps - 1), 0)
            return carry

        lax.fori_loop(0, steps // 2, two_steps, 0)
        if last:
            for shard in range(shards):
                out_ref[shard, own : own + 1, :] = row_total_ref[...]
                out_ref[shard, own + 1 : own + 2, :] = col_total_ref[...]
            move.wait()

    vmem = pl.BlockSpec(memory_space=pltpu.VMEM)
    anywhere = pl.BlockSpec(memory_space=pl.ANY)
    operands = [cols, rows] + ([payload] if chained else [])
    in_specs = [vmem] * len(operands)
    out_shape = [jax.ShapeDtypeStruct((shards, height, row_count), F32)]
    out_specs = [vmem]
    scratch = [
        pltpu.VMEM((col_count, samples), F32),
        pltpu.VMEM((row_count, 2 * slot_width), BF16),
    ]
    if last:
        operands += [totals[0], totals[1], landed]
        in_specs += [vmem, vmem, anywhere]
        out_shape.append(jax.ShapeDtypeStruct(landed.shape, landed.dtype))
        out_specs.append(anywhere)
        scratch.append(pltpu.SemaphoreType.DMA(()))
    return pl.pallas_call(
        kernel,
        out_shape=out_shape,
        in_specs=in_specs,
        out_specs=out_specs,
        scratch_shapes=scratch,
        name="chunk_terms",
    )(*operands)


def body(vectors, partner, next_rows):
    shards = lax.axis_size("samp")
    row_count = vectors.shape[0]
    col_count = partner.shape[0]
    own = col_count // shards
    bounds = [col_count * cut // 16 for cut in CUTS]
    arrived = []
    for low, high in zip(bounds, bounds[1:]):
        arrived.append(from_behind(partner[low:high], "vblk", 1))
    samples = next_rows.shape[1] // shards
    outgoing = next_rows.reshape(next_rows.shape[0], shards, samples).transpose(1, 0, 2)
    landed = lax.all_to_all(outgoing, "samp", split_axis=0, concat_axis=0, tiled=True)
    landed = landed.reshape(-1, samples)
    row_totals = jnp.sum(vectors, axis=1, dtype=F32)[None, :]
    col_totals = jnp.sum(partner, axis=1, dtype=F32)[None, :]
    col_totals = from_behind(col_totals, "vblk", 1)
    height = -(-(own + 2) // 8) * 8
    payload = (shards, height, row_count)
    for i, piece in enumerate(arrived):
        last = i == len(arrived) - 1
        totals = (row_totals, col_totals, own) if last else (None, None, own)
        results = chunk_terms(piece, vectors, bounds[i], payload, totals, landed)
        payload = results[0]
    next_block = results[1]
    summed = jnp.sum(
        lax.all_to_all(payload, "samp", split_axis=0, concat_axis=0, tiled=True), axis=0
    )
    mine = lax.dynamic_slice_in_dim(summed[own + 1], lax.axis_index("samp") * own, own)
    metric = 2.0 * summed[:own] / (summed[own][None, :] + mine[:, None])
    return (metric.T, next_block)


def solution(mesh):
    in_specs = (P("vblk", "samp"), P("vblk", "samp"), P(("vblk", "samp"), None))
    out_specs = (P("vblk", "samp"), P("vblk", "samp"))
    return jax.shard_map(body, mesh=mesh, in_specs=in_specs, out_specs=out_specs, check_vma=False)
```

```python
import jax
import jax.numpy as jnp
from jax import lax
from jax.experimental import pallas as pl
from jax.experimental.pallas import tpu as pltpu
from jax.sharding import PartitionSpec as P


F32 = jnp.float32
BF16 = jnp.bfloat16
CUTS = (0, 2, 6, 11, 16)
DEPTH = 8


def from_behind(value, axis, steps):
    count = lax.axis_size(axis)
    pairs = [(source, (source + steps) % count) for source in range(count)]
    return lax.ppermute(value, axis, pairs)


def tree_sum(terms):
    while len(terms) > 1:
        paired = [terms[i] + terms[i + 1] for i in range(0, len(terms) - 1, 2)]
        terms = paired + terms[len(paired) * 2 :]
    return terms[0]


def largest_divisor(size, limit):
    return max(d for d in range(1, limit + 1) if size % d == 0)


def lane_sums(left, right):
    return lax.dot_general(left, right, (((1,), (1,)), ((), ())), preferred_element_type=F32)


def chunk_terms(cols, rows, first, payload, totals):
    col_count, samples = cols.shape
    row_count = rows.shape[0]
    shards, height, _ = payload if isinstance(payload, tuple) else payload.shape
    own = totals[2]
    last = totals[0] is not None
    halves = 2 if samples % 512 == 0 else 1
    span = samples // halves
    depth = largest_divisor(span // 128, DEPTH)
    width = span // depth
    group = 2
    steps = col_count // group
    slot_width = group * halves * width
    chained = not isinstance(payload, tuple)

    def kernel(*refs):
        refs = list(refs)
        col_ref, row_ref = refs[:2]
        refs = refs[2:]
        old_ref = refs.pop(0) if chained else None
        if last:
            row_total_ref, col_total_ref = refs[:2]
            refs = refs[2:]
        out_ref, wide_ref, part_ref = refs
        wide_ref[...] = col_ref[...].astype(F32)
        if chained:
            out_ref[...] = old_ref[...]
        else:
            out_ref[...] = jnp.zeros_like(out_ref)
        ones = jnp.ones((8, halves * width), BF16)

        def minima(step, slot):
            for half in range(halves):
                start = half * span
                spread = [
                    jnp.broadcast_to(
                        wide_ref[pl.ds(step * group + q, 1), start : start + span], (16, span)
                    ).astype(BF16)
                    for q in range(group)
                ]
                for block in range(0, row_count, 16):
                    for q in range(group):
                        at = slot * slot_width + (q * halves + half) * width
                        part_ref[block : block + 16, at : at + width] = tree_sum(
                            [
                                jnp.minimum(
                                    row_ref[block : block + 16, start + k : start + k + width],
                                    spread[q][:, k : k + width],
                                )
                                for k in range(0, span, width)
                            ]
                        )

        def finish(step, slot):
            for q in range(group):
                at = slot * slot_width + q * halves * width
                line = lane_sums(ones, part_ref[:, at : at + halves * width])
                col = first + step * group + q
                out_ref[col // own, pl.ds(col % own, 1), :] = line[0:1]

        minima(0, 0)

        def two_steps(index, carry):
            finish(2 * index, 0)
            minima(2 * index + 1, 1)
            finish(2 * index + 1, 1)
            minima(jnp.minimum(2 * index + 2, steps - 1), 0)
            return carry

        lax.fori_loop(0, steps // 2, two_steps, 0)
        if last:
            for shard in range(shards):
                out_ref[shard, own : own + 1, :] = row_total_ref[...]
                out_ref[shard, own + 1 : own + 2, :] = col_total_ref[...]

    vmem = pl.BlockSpec(memory_space=pltpu.VMEM)
    operands = [cols, rows] + ([payload] if chained else [])
    in_specs = [vmem] * len(operands)
    scratch = [
        pltpu.VMEM((col_count, samples), F32),
        pltpu.VMEM((row_count, 2 * slot_width), BF16),
    ]
    if last:
        operands += [totals[0], totals[1]]
        in_specs += [vmem, vmem]
    return pl.pallas_call(
        kernel,
        out_shape=jax.ShapeDtypeStruct((shards, height, row_count), F32),
        in_specs=in_specs,
        out_specs=vmem,
        scratch_shapes=scratch,
        name="chunk_terms",
    )(*operands)


def moved(block):
    rows, samples = block.shape
    spec = pl.BlockSpec((rows // 8, samples), lambda i: (i, 0))

    def kernel(in_ref, out_ref):
        out_ref[...] = in_ref[...]

    return pl.pallas_call(
        kernel,
        out_shape=jax.ShapeDtypeStruct(block.shape, block.dtype),
        grid=(8,),
        in_specs=[spec],
        out_specs=spec,
        name="moved",
    )(block)


def body(vectors, partner, next_rows):
    shards = lax.axis_size("samp")
    row_count = vectors.shape[0]
    col_count = partner.shape[0]
    own = col_count // shards
    bounds = [col_count * cut // 16 for cut in CUTS]
    arrived = []
    for low, high in zip(bounds, bounds[1:]):
        arrived.append(from_behind(partner[low:high], "vblk", 1))
    samples = next_rows.shape[1] // shards
    outgoing = next_rows.reshape(next_rows.shape[0], shards, samples).transpose(1, 0, 2)
    landed = lax.all_to_all(outgoing, "samp", split_axis=0, concat_axis=0, tiled=True)
    landed = landed.reshape(-1, samples)
    row_totals = jnp.sum(vectors, axis=1, dtype=F32)[None, :]
    col_totals = jnp.sum(partner, axis=1, dtype=F32)[None, :]
    col_totals = from_behind(col_totals, "vblk", 1)
    height = -(-(own + 2) // 8) * 8
    payload = (shards, height, row_count)
    for i, piece in enumerate(arrived):
        last = i == len(arrived) - 1
        totals = (row_totals, col_totals, own) if last else (None, None, own)
        payload = chunk_terms(piece, vectors, bounds[i], payload, totals)
    gathered = lax.all_to_all(payload, "samp", split_axis=0, concat_axis=0, tiled=True)
    next_block = moved(landed)
    summed = jnp.sum(gathered, axis=0)
    mine = lax.dynamic_slice_in_dim(summed[own + 1], lax.axis_index("samp") * own, own)
    metric = 2.0 * summed[:own] / (summed[own][None, :] + mine[:, None])
    return (metric.T, next_block)


def solution(mesh):
    in_specs = (P("vblk", "samp"), P("vblk", "samp"), P(("vblk", "samp"), None))
    out_specs = (P("vblk", "samp"), P("vblk", "samp"))
    return jax.shard_map(body, mesh=mesh, in_specs=in_specs, out_specs=out_specs, check_vma=False)
```
